16 devices in a mesh: pp: 2 (over z), tp: 8 (over y, x, core).
Axes of the slice: x: 2, y: 2, z: 2, core: 2. Of those that a mesh axis runs over, the one named last changes fastest.
Arguments:
- activations: bfloat16 [384, 28, 28, 384], P(('pp', 'tp'))
- conv_w: bfloat16 [3, 3, 384, 384], P(None, None, 'tp')
- bn_scale: float32 [384], P('tp')
- bn_shift: float32 [384], P('tp')
Outputs:
- output: bfloat16 [384, 28, 28, 384], P('pp', None, None, 'tp')
All inputs are finite; a program needn't handle non-finite values.
Results may differ from the reference program's by a relative error of at most 0.001.
Values are sent between devices in bfloat16 or wider.
A program may use at most 1 GiB of HBM per device.

```python
import math
import jax
import jax.numpy as jnp
from jax import lax

IMAGES = 192
IMG_BLOCK = 192
HEIGHT = 28
WIDTH = 28
C_IN = 384
C_OUT = 384
CONV_DIMS = ("NHWC", "HWIO", "NHWC")


def setup_inputs(seed: int = 0) -> dict:
    base_key = jax.random.key(seed)
    act_key, w_key, scale_key, shift_key = jax.random.split(base_key, 4)
    live_rows = jax.random.normal(act_key, (IMAGES, HEIGHT, WIDTH, C_IN), jnp.float32)
    activations = jnp.concatenate([live_rows, jnp.zeros_like(live_rows)], axis=0).astype(jnp.bfloat16)
    w_scale = 1.0 / math.sqrt(9 * C_IN)
    conv_w = (jax.random.normal(w_key, (3, 3, C_IN, C_OUT), jnp.float32) * w_scale).astype(jnp.bfloat16)
    bn_scale = jax.random.uniform(scale_key, (C_OUT,), jnp.float32, 0.5, 1.5)
    bn_shift = 0.5 * jax.random.normal(shift_key, (C_OUT,), jnp.float32)
    return {"activations": activations, "conv_w": conv_w, "bn_scale": bn_scale, "bn_shift": bn_shift}


def reference(activations, conv_w, bn_scale, bn_shift):
    kernel = conv_w.astype(jnp.float32)
    live_rows = activations[:IMAGES].astype(jnp.float32)
    conv_blocks = live_rows.reshape(IMAGES // IMG_BLOCK, IMG_BLOCK, HEIGHT, WIDTH, C_IN)

    def one_block(x_block):
        pre_act = lax.conv_general_dilated(x_block, kernel, (1, 1), "SAME", dimension_numbers=CONV_DIMS)
        y_val = pre_act * bn_scale + bn_shift
        return jnp.maximum(y_val, 0.0).astype(jnp.bfloat16)

    z_rows = lax.map(one_block, conv_blocks).reshape(IMAGES, HEIGHT, WIDTH, C_OUT)
    return jnp.concatenate([jnp.zeros_like(z_rows), z_rows], axis=0)
```

```python
import functools

import jax
import jax.numpy as jnp
from jax import lax
from jax.experimental import pallas as pl
from jax.experimental.pallas import tpu as pltpu
from jax.sharding import PartitionSpec as P


BF16 = jnp.bfloat16
F32 = jnp.float32
ROWS = 28
COLS = 28
CH = 384
BLK = 48
IMGS = 24
RAW = 8
LIVE = IMGS - RAW
LANES = 128
VMEM_LIMIT = 60 * 1024 * 1024
HEAD = 2
CROSS_CHUNKS = ((0, 16), (16, 12))
LOCAL_CHUNKS = (((0, 28), (28, 28)), ((56, 16), (72, 12), (84, 8), (92, 6)))


def conv_body(meta_ref, *refs, **sizes):
    @pl.when(meta_ref[2] == 1)
    def _():
        conv_step(meta_ref, refs, **sizes)


def conv_step(meta_ref, refs, row0, img0, imgs, step_rows, heights):
    outs = refs[-11:-3]
    pad, col, flip = refs[-3:]
    edge = jnp.zeros((imgs, CH), BF16)
    for j in range(step_rows + 2):
        row = step_rows * pl.program_id(0) + row0 - 1 + j

        @pl.when(jnp.logical_or(row < 0, row >= ROWS))
        def _():
            pad[j, 1 : COLS + 1] = jnp.zeros((COLS, imgs, CH), BF16)

        begin = 0
        for piece, height in enumerate(heights):
            row_ref = refs[piece * (step_rows + 2) + j]

            @pl.when(jnp.logical_and(row >= begin, row < begin + height))
            def _():
                pad[j, 1 : COLS + 1] = row_ref[0, :, img0 : img0 + imgs, :]

            begin += height
        pad[j, 0] = edge
        pad[j, COLS + 1] = edge
    w_ref, scale_ref, shift_ref = refs[len(heights) * (step_rows + 2) :][:3]
    size = step_rows * COLS * imgs
    for a in range(3):
        for b in range(3):
            tap = 3 * a + b
            col[:, tap * CH : (tap + 1) * CH] = pad[a : a + step_rows, b : b + COLS].reshape(size, CH)
    pre = jnp.dot(col[...], w_ref[...], preferred_element_type=F32)
    z_val = jnp.maximum(pre * scale_ref[...] + shift_ref[...], 0.0)
    for g in range(size // LANES):
        group = z_val[g * LANES : (g + 1) * LANES]
        if imgs == RAW:
            group = group.reshape(2, 8, 8, CH).swapaxes(0, 1).reshape(LANES, CH)
            turn = meta_ref[1]
        else:
            turn = meta_ref[1] + 8 * ((7 * (row0 // 2 + pl.program_id(0)) + g) % 2)
        flip[g] = pltpu.roll(group, turn, 0).astype(BF16).T
    for k in range(8):
        start = pl.multiple_of(lax.bitwise_xor(meta_ref[0], k) * BLK, BLK)
        for g in range(size // LANES):
            outs[k][g] = flip[g, pl.ds(start, BLK), :]


def conv_call(meta, pieces, w_full, scale, shift, after, row0, steps, img0, imgs, step_rows):
    size = step_rows * COLS * imgs
    groups = size // LANES

    def row_specs(begin, piece):
        height, _, depth, _ = piece.shape
        return [
            pl.BlockSpec((1, COLS, depth, CH), lambda i, m, j=j: (jnp.clip(step_rows * i * m[2] + row0 - 1 + j - begin, 0, height - 1), 0, 0, 0))
            for j in range(step_rows + 2)
        ]

    def whole(*shape):
        return pl.BlockSpec(shape, lambda i, m: (0,) * len(shape))

    heights = tuple(piece.shape[0] for piece in pieces)
    specs, operands, begin = [], [], 0
    for piece in pieces:
        specs += row_specs(begin, piece)
        operands += [piece] * (step_rows + 2)
        begin += piece.shape[0]
    return pl.pallas_call(
        functools.partial(conv_body, row0=row0, img0=img0, imgs=imgs, step_rows=step_rows, heights=heights),
        grid_spec=pltpu.PrefetchScalarGridSpec(
            num_scalar_prefetch=1,
            grid=(steps,),
            in_specs=specs + [whole(9 * CH, CH), whole(1, CH), whole(1, CH)] + [pl.BlockSpec(memory_space=pl.ANY)] * len(after),
            out_specs=[pl.BlockSpec((groups, BLK, LANES), lambda i, m: (i * m[2], 0, 0))] * 8,
            scratch_shapes=[
                pltpu.VMEM((step_rows + 2, COLS + 2, imgs, CH), BF16),
                pltpu.VMEM((size, 9 * CH), BF16),
                pltpu.VMEM((groups, CH, LANES), BF16),
            ],
        ),
        out_shape=[jax.ShapeDtypeStruct((steps * groups, BLK, LANES), BF16)] * 8,
        compiler_params=pltpu.CompilerParams(vmem_limit_bytes=VMEM_LIMIT),
        cost_estimate=pl.CostEstimate(flops=2 * steps * size * 9 * CH * CH, bytes_accessed=steps * size * CH * 4, transcendentals=0),
    )(meta, *operands, w_full, scale, shift, *after)


def turned_slot(turn):
    lane = lax.broadcasted_iota(jnp.int32, (16, LANES), 1)
    return ((lane // 8 - turn) & 15).astype(F32).astype(BF16)


def merge_body(meta_ref, *refs, aliased):
    z_refs, r_refs = refs[0:6], refs[6:14]
    out = refs[15] if aliased else refs[14]
    z_hold, r_hold = refs[-2:]
    slots = ([], [])
    for d in range(8):
        for hold, some in ((r_hold, (3 * d,)), (z_hold, (3 * d + 1, 3 * d + 2))):
            for tile in range(2):
                inside = [s - 16 * tile for s in some if 16 * tile <= s < 16 * tile + 16]
                if inside:
                    slots[tile].append((hold, d, inside[0], len(inside)))

    def merge_pixels(p, odd):
        turn = 2 * p + odd
        slot = turned_slot(turn)
        masks = []
        for tile in range(2):
            for hold, d, begin, count in slots[tile]:
                mask = slot == begin if count == 1 else jnp.logical_and(slot >= begin, slot <= begin + 1)
                masks.append(mask)
        for r in range(7):
            g = 2 * r + odd
            for row in range(0, BLK, 16):
                at = 0
                for tile in range(2):
                    value = None
                    for hold, d, begin, count in slots[tile]:
                        part = hold[d, r if hold is r_hold else g, row : row + 16, :]
                        value = part if value is None else jnp.where(masks[at], part, value)
                        at += 1
                    value = pltpu.roll(value, (LANES - 8 * turn) & 127, 1)
                    if tile == 0:
                        out[8 * g + p, row : row + 16, 0:LANES] = value
                    else:
                        out[8 * g + p, row : row + 16, LANES:192] = value[:, 0:64]

    @pl.when(meta_ref[2] == 1)
    def _():
        for k in range(8):
            d = lax.bitwise_xor(meta_ref[0], k)
            if k >= 2:
                z_hold[d] = z_refs[k - 2][...]
            r_hold[d] = r_refs[k][...]
        for odd in range(2):

            @pl.loop(0, 8)
            def _(p):
                merge_pixels(p, odd)

    @pl.when(meta_ref[2] == 0)
    def _():
        out[...] = jnp.zeros(out.shape, BF16)


def merge_call(meta, z_parts, r_parts, dst, row0, rows):
    quad = row0 // 4
    in_specs = [pl.BlockSpec((14, BLK, LANES), lambda i, m: (i * m[2], 0, 0))] * 6
    in_specs += [pl.BlockSpec((7, BLK, LANES), lambda i, m: (quad + i * m[2], 0, 0))] * 8
    operands = [*z_parts, *r_parts]
    aliases = {}
    if dst is not None:
        in_specs.append(pl.BlockSpec(memory_space=pl.ANY))
        operands.append(dst)
        aliases = {15: 0}
    return pl.pallas_call(
        functools.partial(merge_body, aliased=dst is not None),
        grid_spec=pltpu.PrefetchScalarGridSpec(
            num_scalar_prefetch=1,
            grid=(rows // 4,),
            in_specs=in_specs,
            out_specs=pl.BlockSpec((112, BLK, 192), lambda i, m: (quad + i, 0, 0)),
            scratch_shapes=[pltpu.VMEM((8, 14, BLK, LANES), BF16), pltpu.VMEM((8, 7, BLK, LANES), BF16)],
        ),
        out_shape=jax.ShapeDtypeStruct((ROWS * COLS, BLK, 192), BF16),
        input_output_aliases=aliases,
        compiler_params=pltpu.CompilerParams(vmem_limit_bytes=VMEM_LIMIT),
        cost_estimate=pl.CostEstimate(flops=rows * 10**7, bytes_accessed=rows * COLS * BLK * 192 * 4, transcendentals=0),
    )(meta, *operands)


def patch_body(meta_ref, first, second, before, result, both_buf, part_buf, both_sem, in_sem, out_sem, *, group0):
    steps = part_buf.shape[0]

    def pixels(i):
        return pl.ds(pl.multiple_of(8 * group0 + 16 * i, 16), 16)

    def load(i):
        return pltpu.make_async_copy(before.at[pixels(i)], part_buf.at[i], in_sem.at[i])

    def store(i):
        return pltpu.make_async_copy(part_buf.at[i], result.at[pixels(i)], out_sem.at[i])

    @pl.when(meta_ref[2] == 1)
    def _():
        arrivals = [pltpu.make_async_copy(ref, both_buf.at[k], both_sem.at[k]) for k, ref in enumerate((first, second))]
        for arrival in arrivals:
            arrival.start()

        @pl.loop(0, steps)
        def _(i):
            load(i).start()

        begins = [3 * lax.bitwise_xor(meta_ref[0], k) + 1 for k in range(2)]
        lane = lax.broadcasted_iota(jnp.int32, (16, LANES), 1)
        keep = []
        for tile in range(2):
            ahead = [lane // 8 + 16 * tile - begin for begin in begins]
            mine = jnp.where(jnp.logical_or((ahead[0] & -2) == 0, (ahead[1] & -2) == 0), 1.0, 0.0)
            keep.append(mine.astype(BF16) == 1.0)
        for arrival in arrivals:
            arrival.wait()

        @pl.loop(0, steps)
        def _(i):
            load(i).wait()
            for odd in range(2):
                for p in range(8):
                    turn = 2 * p + odd
                    from_second = turned_slot(turn + begins[1]) <= 1
                    pixel = 8 * odd + p
                    for row in range(0, BLK, 16):
                        some = pl.ds(row, 16)
                        both = jnp.where(from_second, both_buf[1, 2 * i + odd, some, :], both_buf[0, 2 * i + odd, some, :])
                        both = pltpu.roll(both, (LANES - 8 * turn) & 127, 1)
                        part_buf[i, pixel, some, 0:LANES] = jnp.where(keep[0], both, part_buf[i, pixel, some, 0:LANES])
                        high = jnp.where(keep[1][:, 0:64], both[:, 0:64], part_buf[i, pixel, some, LANES:192])
                        part_buf[i, pixel, some, LANES:192] = high
            store(i).start()

        @pl.loop(0, steps)
        def _(i):
            store(i).wait()


def patch_call(meta, first, second, result, group0, groups):
    assert group0 % 2 == 0 and groups % 2 == 0
    steps = groups // 2
    return pl.pallas_call(
        functools.partial(patch_body, group0=group0),
        in_specs=[pl.BlockSpec(memory_space=pltpu.SMEM)] + [pl.BlockSpec(memory_space=pltpu.HBM)] * 3,
        out_specs=pl.BlockSpec(memory_space=pltpu.HBM),
        out_shape=jax.ShapeDtypeStruct((ROWS * COLS, BLK, 192), BF16),
        scratch_shapes=[
            pltpu.VMEM((2, groups, BLK, LANES), BF16),
            pltpu.VMEM((steps, 16, BLK, 192), BF16),
            pltpu.SemaphoreType.DMA((2,)),
            pltpu.SemaphoreType.DMA((steps,)),
            pltpu.SemaphoreType.DMA((steps,)),
        ],
        input_output_aliases={3: 0},
        compiler_params=pltpu.CompilerParams(vmem_limit_bytes=VMEM_LIMIT),
        cost_estimate=pl.CostEstimate(flops=groups * 10**6, bytes_accessed=groups * 8 * BLK * 192 * 4, transcendentals=0),
    )(meta, first, second, result)


def solution(mesh):
    def cross_pairs(k):
        return [(t, 8 + (t ^ k)) for t in range(8)]

    def late_pairs(k):
        return [(8 + t, 8 + (t ^ k)) for t in range(8)]

    def block_step(act_block, w_shard, scale_shard, shift_shard):
        pp, tp = lax.axis_index("pp"), lax.axis_index("tp")
        axes = ("pp", "tp")
        x_rows = jnp.transpose(act_block, (1, 2, 0, 3))
        raw_head = lax.ppermute(x_rows[:HEAD, :, :RAW], axes, cross_pairs(0))
        raw_tail = lax.ppermute(x_rows[HEAD:, :, :RAW], axes, cross_pairs(0))
        w_full = jnp.concatenate([lax.all_gather(w_shard[a], "tp", axis=1, tiled=True) for a in range(3)], axis=0)
        w_full = w_full.reshape(9 * CH, CH)
        affine = lax.all_gather(jnp.stack([scale_shard, shift_shard]), "tp", axis=1, tiled=True)
        scale, shift = affine[0:1], affine[1:2]
        z_meta = jnp.stack([tp, 8 * (3 * tp + 1), 1 - pp]).astype(jnp.int32)
        r_meta = jnp.stack([tp, 24 * tp, pp]).astype(jnp.int32)
        r_parts = conv_call(r_meta, (raw_head, raw_tail), w_full, scale, shift, (), 0, 7, 0, RAW, 4)
        r_recv = [r_parts[0]] + [lax.ppermute(r_parts[k], axes, late_pairs(k)) for k in range(1, 8)]
        z_recv, local_recv = [], []
        after = ()
        for c, (row0, rows) in enumerate(CROSS_CHUNKS):
            z_parts = conv_call(z_meta, (x_rows,), w_full, scale, shift, after, row0, rows // 2, RAW, LIVE, 2)
            for begin, count in LOCAL_CHUNKS[c]:
                some = slice(begin - row0 // 2 * 7, begin + count - row0 // 2 * 7)
                local_recv.append((begin, count, [lax.ppermute(z_parts[k][some], axes, cross_pairs(k)) for k in range(2)]))
            z_recv.append([lax.ppermute(z_parts[k], axes, cross_pairs(k)) for k in range(2, 8)])
            after = (z_parts[0],)
        result = None
        for (row0, rows), z_parts in zip(CROSS_CHUNKS, z_recv):
            result = merge_call(r_meta, z_parts, r_recv, result, row0, rows)
        for group0, groups, (first, second) in local_recv:
            result = patch_call(r_meta, first, second, result, group0, groups)
        return jnp.transpose(result.reshape(ROWS, COLS, BLK, 192), (3, 0, 1, 2))

    return jax.shard_map(block_step, mesh=mesh, in_specs=(P(("pp", "tp")), P(None, None, "tp", None), P("tp"), P("tp")), out_specs=P("pp", None, None, "tp"), check_vma=False)
```

```python
import functools

import jax
import jax.numpy as jnp
from jax import lax
from jax.experimental import pallas as pl
from jax.experimental.pallas import tpu as pltpu
from jax.sharding import PartitionSpec as P


BF16 = jnp.bfloat16
F32 = jnp.float32
ROWS = 28
COLS = 28
CH = 384
BLK = 48
IMGS = 24
RAW = 8
LIVE = IMGS - RAW
LANES = 128
VMEM_LIMIT = 60 * 1024 * 1024
PATCH_VMEM_LIMIT = 16 * 1024 * 1024
HEAD = 2
FETCHED = 2
CROSS_CHUNKS = ((0, 16), (16, 12))
LOCAL_CHUNKS = (((0, 28), (28, 28)), ((56, 16), (72, 14), (86, 6), (92, 6)))


def conv_body(meta_ref, *refs, **sizes):
    @pl.when(meta_ref[2] == 1)
    def _():
        conv_step(meta_ref, refs, **sizes)


def conv_step(meta_ref, refs, row0, img0, imgs, step_rows, heights):
    outs = refs[-11:-3]
    pad, col, flip = refs[-3:]
    edge = jnp.zeros((imgs, CH), BF16)
    for j in range(step_rows + 2):
        row = step_rows * pl.program_id(0) + row0 - 1 + j

        @pl.when(jnp.logical_or(row < 0, row >= ROWS))
        def _():
            pad[j, 1 : COLS + 1] = jnp.zeros((COLS, imgs, CH), BF16)

        begin = 0
        for piece, height in enumerate(heights):
            row_ref = refs[piece * (step_rows + 2) + j]

            @pl.when(jnp.logical_and(row >= begin, row < begin + height))
            def _():
                pad[j, 1 : COLS + 1] = row_ref[0, :, img0 : img0 + imgs, :]

            begin += height
        pad[j, 0] = edge
        pad[j, COLS + 1] = edge
    w_ref, scale_ref, shift_ref = refs[len(heights) * (step_rows + 2) :][:3]
    size = step_rows * COLS * imgs
    for a in range(3):
        for b in range(3):
            tap = 3 * a + b
            col[:, tap * CH : (tap + 1) * CH] = pad[a : a + step_rows, b : b + COLS].reshape(size, CH)
    pre = jnp.dot(col[...], w_ref[...], preferred_element_type=F32)
    z_val = jnp.maximum(pre * scale_ref[...] + shift_ref[...], 0.0)
    for g in range(size // LANES):
        group = z_val[g * LANES : (g + 1) * LANES]
        if imgs == RAW:
            group = group.reshape(2, 8, 8, CH).swapaxes(0, 1).reshape(LANES, CH)
            turn = meta_ref[1]
        else:
            turn = meta_ref[1] + 8 * ((7 * (row0 // 2 + pl.program_id(0)) + g) % 2)
        flip[g] = pltpu.roll(group, turn, 0).astype(BF16).T
    for k in range(8):
        start = pl.multiple_of(lax.bitwise_xor(meta_ref[0], k) * BLK, BLK)
        for g in range(size // LANES):
            outs[k][g] = flip[g, pl.ds(start, BLK), :]


def conv_call(meta, pieces, w_full, scale, shift, after, row0, steps, img0, imgs, step_rows):
    size = step_rows * COLS * imgs
    groups = size // LANES

    def row_specs(begin, piece):
        height, _, depth, _ = piece.shape
        return [
            pl.BlockSpec((1, COLS, depth, CH), lambda i, m, j=j: (jnp.clip(step_rows * i * m[2] + row0 - 1 + j - begin, 0, height - 1), 0, 0, 0))
            for j in range(step_rows + 2)
        ]

    def whole(*shape):
        return pl.BlockSpec(shape, lambda i, m: (0,) * len(shape))

    heights = tuple(piece.shape[0] for piece in pieces)
    specs, operands, begin = [], [], 0
    for piece in pieces:
        specs += row_specs(begin, piece)
        operands += [piece] * (step_rows + 2)
        begin += piece.shape[0]
    return pl.pallas_call(
        functools.partial(conv_body, row0=row0, img0=img0, imgs=imgs, step_rows=step_rows, heights=heights),
        grid_spec=pltpu.PrefetchScalarGridSpec(
            num_scalar_prefetch=1,
            grid=(steps,),
            in_specs=specs + [whole(9 * CH, CH), whole(1, CH), whole(1, CH)] + [pl.BlockSpec(memory_space=pl.ANY)] * len(after),
            out_specs=[pl.BlockSpec((groups, BLK, LANES), lambda i, m: (i * m[2], 0, 0))] * 8,
            scratch_shapes=[
                pltpu.VMEM((step_rows + 2, COLS + 2, imgs, CH), BF16),
                pltpu.VMEM((size, 9 * CH), BF16),
                pltpu.VMEM((groups, CH, LANES), BF16),
            ],
        ),
        out_shape=[jax.ShapeDtypeStruct((steps * groups, BLK, LANES), BF16)] * 8,
        compiler_params=pltpu.CompilerParams(vmem_limit_bytes=VMEM_LIMIT),
        cost_estimate=pl.CostEstimate(flops=2 * steps * size * 9 * CH * CH, bytes_accessed=steps * size * CH * 4, transcendentals=0),
    )(meta, *operands, w_full, scale, shift, *after)


def turned_slot(turn):
    lane = lax.broadcasted_iota(jnp.int32, (16, LANES), 1)
    return ((lane // 8 - turn) & 15).astype(F32).astype(BF16)


def merge_body(meta_ref, *refs, aliased):
    z_refs, r_refs = refs[0:6], refs[6:14]
    out = refs[15] if aliased else refs[14]
    z_hold, r_hold = refs[-2:]
    slots = ([], [])
    for d in range(8):
        for hold, some in ((r_hold, (3 * d,)), (z_hold, (3 * d + 1, 3 * d + 2))):
            for tile in range(2):
                inside = [s - 16 * tile for s in some if 16 * tile <= s < 16 * tile + 16]
                if inside:
                    slots[tile].append((hold, d, inside[0], len(inside)))

    def merge_pixels(p, odd):
        turn = 2 * p + odd
        slot = turned_slot(turn)
        masks = []
        for tile in range(2):
            for hold, d, begin, count in slots[tile]:
                mask = slot == begin if count == 1 else jnp.logical_and(slot >= begin, slot <= begin + 1)
                masks.append(mask)
        for r in range(7):
            g = 2 * r + odd
            for row in range(0, BLK, 16):
                at = 0
                for tile in range(2):
                    value = None
                    for hold, d, begin, count in slots[tile]:
                        part = hold[d, r if hold is r_hold else g, row : row + 16, :]
                        value = part if value is None else jnp.where(masks[at], part, value)
                        at += 1
                    value = pltpu.roll(value, (LANES - 8 * turn) & 127, 1)
                    if tile == 0:
                        out[8 * g + p, row : row + 16, 0:LANES] = value
                    else:
                        out[8 * g + p, row : row + 16, LANES:192] = value[:, 0:64]

    @pl.when(meta_ref[2] == 1)
    def _():
        for k in range(8):
            d = lax.bitwise_xor(meta_ref[0], k)
            if k >= 2:
                z_hold[d] = z_refs[k - 2][...]
            r_hold[d] = r_refs[k][...]
        for odd in range(2):

            @pl.loop(0, 8)
            def _(p):
                merge_pixels(p, odd)

    @pl.when(meta_ref[2] == 0)
    def _():
        out[...] = jnp.zeros(out.shape, BF16)


def merge_call(meta, z_parts, r_parts, dst, row0, rows):
    quad = row0 // 4
    in_specs = [pl.BlockSpec((14, BLK, LANES), lambda i, m: (i * m[2], 0, 0))] * 6
    in_specs += [pl.BlockSpec((7, BLK, LANES), lambda i, m: (quad + i * m[2], 0, 0))] * 8
    operands = [*z_parts, *r_parts]
    aliases = {}
    if dst is not None:
        in_specs.append(pl.BlockSpec(memory_space=pl.ANY))
        operands.append(dst)
        aliases = {15: 0}
    return pl.pallas_call(
        functools.partial(merge_body, aliased=dst is not None),
        grid_spec=pltpu.PrefetchScalarGridSpec(
            num_scalar_prefetch=1,
            grid=(rows // 4,),
            in_specs=in_specs,
            out_specs=pl.BlockSpec((112, BLK, 192), lambda i, m: (quad + i, 0, 0)),
            scratch_shapes=[pltpu.VMEM((8, 14, BLK, LANES), BF16), pltpu.VMEM((8, 7, BLK, LANES), BF16)],
        ),
        out_shape=jax.ShapeDtypeStruct((ROWS * COLS, BLK, 192), BF16),
        input_output_aliases=aliases,
        compiler_params=pltpu.CompilerParams(vmem_limit_bytes=VMEM_LIMIT),
        cost_estimate=pl.CostEstimate(flops=rows * 10**7, bytes_accessed=rows * COLS * BLK * 192 * 4, transcendentals=0),
    )(meta, *operands)


def patch_body(meta_ref, first, second, *refs, group0, steps, ahead, given):
    refs = list(refs)
    part_buf = refs.pop(0) if given else None
    before, result = refs.pop(0), refs.pop(0)
    fetched, fetch_sem = (refs.pop(0), refs.pop(-1)) if ahead else (None, None)
    out_buf, out_sem = refs[:2]
    if not given:
        both_buf, both_sem, in_sem = refs[2:]
        part_buf = out_buf

    def pixels(start, i):
        return pl.ds(pl.multiple_of(8 * start + 16 * i, 16), 16)

    def load(i):
        return pltpu.make_async_copy(before.at[pixels(group0, i)], part_buf.at[i], in_sem.at[i])

    def store(i):
        return pltpu.make_async_copy(out_buf.at[i], result.at[pixels(group0, i)], out_sem.at[i])

    def fetch(i):
        return pltpu.make_async_copy(before.at[pixels(ahead[0], i)], fetched.at[i], fetch_sem.at[i])

    @pl.when(meta_ref[2] == 1)
    def _():
        if not given:
            arrivals = [pltpu.make_async_copy(ref, both_buf.at[k], both_sem.at[k]) for k, ref in enumerate((first, second))]
            for arrival in arrivals:
                arrival.start()

            @pl.loop(0, steps)
            def _(i):
                load(i).start()

        if ahead:
            for i in range(ahead[1]):
                fetch(i).start()

        begins = [3 * lax.bitwise_xor(meta_ref[0], k) + 1 for k in range(2)]
        lane = lax.broadcasted_iota(jnp.int32, (16, LANES), 1)
        keep = []
        for tile in range(2):
            past = [lane // 8 + 16 * tile - begin for begin in begins]
            mine = jnp.where(jnp.logical_or((past[0] & -2) == 0, (past[1] & -2) == 0), 1.0, 0.0)
            keep.append(mine.astype(BF16) == 1.0)
        if not given:
            for arrival in arrivals:
                arrival.wait()

        @pl.loop(0, steps)
        def _(i):
            if not given:
                load(i).wait()
            for odd in range(2):
                for p in range(8):
                    turn = 2 * p + odd
                    from_second = turned_slot(turn + begins[1]) <= 1
                    pixel = 8 * odd + p
                    for row in range(0, BLK, 16):
                        some = pl.ds(row, 16)
                        if given:
                            pair = [ref[2 * i + odd, some, :] for ref in (first, second)]
                        else:
                            pair = [both_buf[k, 2 * i + odd, some, :] for k in range(2)]
                        both = jnp.where(from_second, pair[1], pair[0])
                        both = pltpu.roll(both, (LANES - 8 * turn) & 127, 1)
                        out_buf[i, pixel, some, 0:LANES] = jnp.where(keep[0], both, part_buf[i, pixel, some, 0:LANES])
                        high = jnp.where(keep[1][:, 0:64], both[:, 0:64], part_buf[i, pixel, some, LANES:192])
                        out_buf[i, pixel, some, LANES:192] = high
            store(i).start()

        @pl.loop(0, steps)
        def _(i):
            store(i).wait()

        if ahead:
            for i in range(ahead[1]):
                fetch(i).wait()


def patch_call(meta, first, second, result, group0, groups, ahead, part):
    assert group0 % 2 == 0 and groups % 2 == 0
    steps = groups // 2
    given = part is not None
    hbm, vmem = pl.BlockSpec(memory_space=pltpu.HBM), pl.BlockSpec(memory_space=pltpu.VMEM)
    in_specs = [pl.BlockSpec(memory_space=pltpu.SMEM)] + ([vmem] * 3 if given else [hbm] * 2) + [hbm]
    operands = [meta, first, second] + ([part] if given else []) + [result]
    out_specs, out_shape = [hbm], [jax.ShapeDtypeStruct((ROWS * COLS, BLK, 192), BF16)]
    scratch = [pltpu.VMEM((steps, 16, BLK, 192), BF16), pltpu.SemaphoreType.DMA((steps,))]
    if not given:
        scratch += [pltpu.VMEM((2, groups, BLK, LANES), BF16), pltpu.SemaphoreType.DMA((2,)), pltpu.SemaphoreType.DMA((steps,))]
    if ahead:
        ahead = (ahead[0], ahead[1] // 2)
        out_specs.append(vmem)
        out_shape.append(pltpu.VMEM((ahead[1], 16, BLK, 192), BF16))
        scratch.append(pltpu.SemaphoreType.DMA((ahead[1],)))
    out = pl.pallas_call(
        functools.partial(patch_body, group0=group0, steps=steps, ahead=ahead, given=given),
        in_specs=in_specs,
        out_specs=out_specs,
        out_shape=out_shape,
        scratch_shapes=scratch,
        input_output_aliases={len(operands) - 1: 0},
        compiler_params=pltpu.CompilerParams(vmem_limit_bytes=PATCH_VMEM_LIMIT),
        cost_estimate=pl.CostEstimate(flops=groups * 10**6, bytes_accessed=groups * 8 * BLK * 192 * 4, transcendentals=0),
    )(*operands)
    return out if ahead else out[0]


def solution(mesh):
    def cross_pairs(k):
        return [(t, 8 + (t ^ k)) for t in range(8)]

    def late_pairs(k):
        return [(8 + t, 8 + (t ^ k)) for t in range(8)]

    def block_step(act_block, w_shard, scale_shard, shift_shard):
        pp, tp = lax.axis_index("pp"), lax.axis_index("tp")

        def send(value, pairs):
            return lax.ppermute(value, ("pp", "tp"), pairs)

        x_rows = jnp.transpose(act_block, (1, 2, 0, 3))
        raw_head = send(x_rows[:HEAD, :, :RAW], cross_pairs(0))
        raw_tail = send(x_rows[HEAD:, :, :RAW], cross_pairs(0))
        w_full = jnp.concatenate([lax.all_gather(w_shard[a], "tp", axis=1, tiled=True) for a in range(3)], axis=0)
        w_full = w_full.reshape(9 * CH, CH)
        affine = lax.all_gather(jnp.stack([scale_shard, shift_shard]), "tp", axis=1, tiled=True)
        scale, shift = affine[0:1], affine[1:2]
        z_meta = jnp.stack([tp, 8 * (3 * tp + 1), 1 - pp]).astype(jnp.int32)
        r_meta = jnp.stack([tp, 24 * tp, pp]).astype(jnp.int32)

        def live(c, after):
            row0, rows = CROSS_CHUNKS[c]
            return conv_call(z_meta, (x_rows,), w_full, scale, shift, after, row0, rows // 2, RAW, LIVE, 2)

        def send_local(c, z_parts):
            base = CROSS_CHUNKS[c][0] // 2 * 7
            return [(g, n, [send(z_parts[k][g - base : g - base + n], cross_pairs(k)) for k in range(2)]) for g, n in LOCAL_CHUNKS[c]]

        def send_cross(z_parts):
            return [send(z_parts[k], cross_pairs(k)) for k in range(2, 8)]

        z_parts = live(0, ())
        local_recv = send_local(0, z_parts)
        z_recv = [send_cross(z_parts)]
        r_parts = conv_call(r_meta, (raw_head, raw_tail), w_full, scale, shift, (), 0, 7, 0, RAW, 4)
        r_recv = [r_parts[0]] + [send(r_parts[k], late_pairs(k)) for k in range(1, 8)]
        z_parts = live(1, (z_parts[0],))
        z_recv.append(send_cross(z_parts))
        local_recv += send_local(1, z_parts)
        result = None
        for (row0, rows), z_parts in zip(CROSS_CHUNKS, z_recv):
            result = merge_call(r_meta, z_parts, r_recv, result, row0, rows)
        parts = {}
        for n, (group0, groups, (first, second)) in enumerate(local_recv):
            ahead = local_recv[n + 2][:2] if n + 2 >= len(local_recv) - FETCHED and n + 2 < len(local_recv) else None
            result = patch_call(r_meta, first, second, result, group0, groups, ahead, parts.get(n))
            if ahead:
                result, parts[n + 2] = result
        return jnp.transpose(result.reshape(ROWS, COLS, BLK, 192), (3, 0, 1, 2))

    return jax.shard_map(block_step, mesh=mesh, in_specs=(P(("pp", "tp")), P(None, None, "tp", None), P("tp"), P("tp")), out_specs=P("pp", None, None, "tp"), check_vma=False)
```

```python
import functools

import jax
import jax.numpy as jnp
from jax import lax
from jax.experimental import pallas as pl
from jax.experimental.pallas import tpu as pltpu
from jax.sharding import PartitionSpec as P


BF16 = jnp.bfloat16
F32 = jnp.float32
ROWS = 28
COLS = 28
CH = 384
BLK = 48
IMGS = 24
RAW = 8
LIVE = IMGS - RAW
LANES = 128
VMEM_LIMIT = 60 * 1024 * 1024
PATCH_VMEM_LIMIT = 16 * 1024 * 1024
HEAD = 2
FETCHED = 3
CROSS_CHUNKS = ((0, 16), (16, 12))
LOCAL_CHUNKS = (((0, 28), (28, 28)), ((56, 16), (72, 14), (86, 6), (92, 6)))


def head_body(x_ref, out, sem):
    @pl.when(lax.axis_index("pp") == 0)
    def _():
        copy = pltpu.make_async_copy(x_ref.at[pl.ds(0, HEAD), :, pl.ds(0, RAW), :], out, sem)
        copy.start()
        copy.wait()


def head_call(x_rows):
    return pl.pallas_call(
        head_body,
        in_specs=[pl.BlockSpec(memory_space=pltpu.HBM)],
        out_specs=pl.BlockSpec(memory_space=pltpu.VMEM),
        out_shape=pltpu.VMEM((HEAD, COLS, RAW, CH), BF16),
        scratch_shapes=[pltpu.SemaphoreType.DMA],
        compiler_params=pltpu.CompilerParams(vmem_limit_bytes=PATCH_VMEM_LIMIT),
        cost_estimate=pl.CostEstimate(flops=1000, bytes_accessed=HEAD * COLS * RAW * CH * 2, transcendentals=0),
        name="head",
    )(pltpu.with_memory_space_constraint(x_rows, pltpu.HBM))


def conv_body(meta_ref, *refs, **sizes):
    @pl.when(meta_ref[2] == 1)
    def _():
        conv_step(meta_ref, refs, **sizes)


def conv_step(meta_ref, refs, row0, img0, imgs, step_rows, heights):
    outs = refs[-11:-3]
    pad, col, flip = refs[-3:]
    edge = jnp.zeros((imgs, CH), BF16)
    for j in range(step_rows + 2):
        row = step_rows * pl.program_id(0) + row0 - 1 + j

        @pl.when(jnp.logical_or(row < 0, row >= ROWS))
        def _():
            pad[j, 1 : COLS + 1] = jnp.zeros((COLS, imgs, CH), BF16)

        begin = 0
        for piece, height in enumerate(heights):
            row_ref = refs[piece * (step_rows + 2) + j]

            @pl.when(jnp.logical_and(row >= begin, row < begin + height))
            def _():
                pad[j, 1 : COLS + 1] = row_ref[0, :, img0 : img0 + imgs, :]

            begin += height
        pad[j, 0] = edge
        pad[j, COLS + 1] = edge
    w_ref, scale_ref, shift_ref = refs[len(heights) * (step_rows + 2) :][:3]
    size = step_rows * COLS * imgs
    for a in range(3):
        for b in range(3):
            tap = 3 * a + b
            col[:, tap * CH : (tap + 1) * CH] = pad[a : a + step_rows, b : b + COLS].reshape(size, CH)
    pre = jnp.dot(col[...], w_ref[...], preferred_element_type=F32)
    z_val = jnp.maximum(pre * scale_ref[...] + shift_ref[...], 0.0)
    for g in range(size // LANES):
        group = z_val[g * LANES : (g + 1) * LANES]
        if imgs == RAW:
            group = group.reshape(2, 8, 8, CH).swapaxes(0, 1).reshape(LANES, CH)
            turn = meta_ref[1]
        else:
            turn = meta_ref[1] + 8 * ((7 * (row0 // 2 + pl.program_id(0)) + g) % 2)
        flip[g] = pltpu.roll(group, turn, 0).astype(BF16).T
    for k in range(8):
        start = pl.multiple_of(lax.bitwise_xor(meta_ref[0], k) * BLK, BLK)
        for g in range(size // LANES):
            outs[k][g] = flip[g, pl.ds(start, BLK), :]


def conv_call(meta, pieces, w_full, scale, shift, after, row0, steps, img0, imgs, step_rows):
    size = step_rows * COLS * imgs
    groups = size // LANES

    def row_specs(begin, piece):
        height, _, depth, _ = piece.shape
        return [
            pl.BlockSpec((1, COLS, depth, CH), lambda i, m, j=j: (jnp.clip(step_rows * i * m[2] + row0 - 1 + j - begin, 0, height - 1), 0, 0, 0))
            for j in range(step_rows + 2)
        ]

    def whole(*shape):
        return pl.BlockSpec(shape, lambda i, m: (0,) * len(shape))

    heights = tuple(piece.shape[0] for piece in pieces)
    specs, operands, begin = [], [], 0
    for piece in pieces:
        specs += row_specs(begin, piece)
        operands += [piece] * (step_rows + 2)
        begin += piece.shape[0]
    return pl.pallas_call(
        functools.partial(conv_body, row0=row0, img0=img0, imgs=imgs, step_rows=step_rows, heights=heights),
        grid_spec=pltpu.PrefetchScalarGridSpec(
            num_scalar_prefetch=1,
            grid=(steps,),
            in_specs=specs + [whole(9 * CH, CH), whole(1, CH), whole(1, CH)] + [pl.BlockSpec(memory_space=pl.ANY)] * len(after),
            out_specs=[pl.BlockSpec((groups, BLK, LANES), lambda i, m: (i * m[2], 0, 0))] * 8,
            scratch_shapes=[
                pltpu.VMEM((step_rows + 2, COLS + 2, imgs, CH), BF16),
                pltpu.VMEM((size, 9 * CH), BF16),
                pltpu.VMEM((groups, CH, LANES), BF16),
            ],
        ),
        out_shape=[jax.ShapeDtypeStruct((steps * groups, BLK, LANES), BF16)] * 8,
        compiler_params=pltpu.CompilerParams(vmem_limit_bytes=VMEM_LIMIT),
        cost_estimate=pl.CostEstimate(flops=2 * steps * size * 9 * CH * CH, bytes_accessed=steps * size * CH * 4, transcendentals=0),
    )(meta, *operands, w_full, scale, shift, *after)


def turned_slot(turn):
    lane = lax.broadcasted_iota(jnp.int32, (16, LANES), 1)
    return ((lane // 8 - turn) & 15).astype(F32).astype(BF16)


def merge_body(meta_ref, *refs, aliased):
    z_refs, r_refs = refs[0:6], refs[6:14]
    out = refs[15] if aliased else refs[14]
    z_hold, r_hold = refs[-2:]
    slots = ([], [])
    for d in range(8):
        for hold, some in ((r_hold, (3 * d,)), (z_hold, (3 * d + 1, 3 * d + 2))):
            for tile in range(2):
                inside = [s - 16 * tile for s in some if 16 * tile <= s < 16 * tile + 16]
                if inside:
                    slots[tile].append((hold, d, inside[0], len(inside)))

    def merge_pixels(p, odd):
        turn = 2 * p + odd
        slot = turned_slot(turn)
        masks = []
        for tile in range(2):
            for hold, d, begin, count in slots[tile]:
                mask = slot == begin if count == 1 else jnp.logical_and(slot >= begin, slot <= begin + 1)
                masks.append(mask)
        for r in range(7):
            g = 2 * r + odd
            for row in range(0, BLK, 16):
                at = 0
                for tile in range(2):
                    value = None
                    for hold, d, begin, count in slots[tile]:
                        part = hold[d, r if hold is r_hold else g, row : row + 16, :]
                        value = part if value is None else jnp.where(masks[at], part, value)
                        at += 1
                    value = pltpu.roll(value, (LANES - 8 * turn) & 127, 1)
                    if tile == 0:
                        out[8 * g + p, row : row + 16, 0:LANES] = value
                    else:
                        out[8 * g + p, row : row + 16, LANES:192] = value[:, 0:64]

    @pl.when(meta_ref[2] == 1)
    def _():
        for k in range(8):
            d = lax.bitwise_xor(meta_ref[0], k)
            if k >= 2:
                z_hold[d] = z_refs[k - 2][...]
            r_hold[d] = r_refs[k][...]
        for odd in range(2):

            @pl.loop(0, 8)
            def _(p):
                merge_pixels(p, odd)

    @pl.when(meta_ref[2] == 0)
    def _():
        out[...] = jnp.zeros(out.shape, BF16)


def merge_call(meta, z_parts, r_parts, dst, row0, rows):
    quad = row0 // 4
    in_specs = [pl.BlockSpec((14, BLK, LANES), lambda i, m: (i * m[2], 0, 0))] * 6
    in_specs += [pl.BlockSpec((7, BLK, LANES), lambda i, m: (quad + i * m[2], 0, 0))] * 8
    operands = [*z_parts, *r_parts]
    aliases = {}
    if dst is not None:
        in_specs.append(pl.BlockSpec(memory_space=pl.ANY))
        operands.append(dst)
        aliases = {15: 0}
    return pl.pallas_call(
        functools.partial(merge_body, aliased=dst is not None),
        grid_spec=pltpu.PrefetchScalarGridSpec(
            num_scalar_prefetch=1,
            grid=(rows // 4,),
            in_specs=in_specs,
            out_specs=pl.BlockSpec((112, BLK, 192), lambda i, m: (quad + i, 0, 0)),
            scratch_shapes=[pltpu.VMEM((8, 14, BLK, LANES), BF16), pltpu.VMEM((8, 7, BLK, LANES), BF16)],
        ),
        out_shape=jax.ShapeDtypeStruct((ROWS * COLS, BLK, 192), BF16),
        input_output_aliases=aliases,
        compiler_params=pltpu.CompilerParams(vmem_limit_bytes=VMEM_LIMIT),
        cost_estimate=pl.CostEstimate(flops=rows * 10**7, bytes_accessed=rows * COLS * BLK * 192 * 4, transcendentals=0),
    )(meta, *operands)


def patch_body(first, second, *refs, group0, steps, ahead, given):
    refs = list(refs)
    part_buf = refs.pop(0) if given else None
    before, result = refs.pop(0), refs.pop(0)
    fetched, fetch_sem = (refs.pop(0), refs.pop(-1)) if ahead else (None, None)
    out_buf, out_sem = refs[:2]
    if not given:
        both_buf, both_sem, in_sem = refs[2:]
        part_buf = out_buf

    def pixels(start, i):
        return pl.ds(pl.multiple_of(8 * start + 16 * i, 16), 16)

    def load(i):
        return pltpu.make_async_copy(before.at[pixels(group0, i)], part_buf.at[i], in_sem.at[i])

    def store(i):
        return pltpu.make_async_copy(out_buf.at[i], result.at[pixels(group0, i)], out_sem.at[i])

    def fetch(i):
        return pltpu.make_async_copy(before.at[pixels(ahead[0], i)], fetched.at[i], fetch_sem.at[i])

    @pl.when(lax.axis_index("pp") == 1)
    def _():
        if not given:
            arrivals = [pltpu.make_async_copy(ref, both_buf.at[k], both_sem.at[k]) for k, ref in enumerate((first, second))]
            for arrival in arrivals:
                arrival.start()

            @pl.loop(0, steps)
            def _(i):
                load(i).start()

        if ahead:
            for i in range(ahead[1]):
                fetch(i).start()

        begins = [3 * lax.bitwise_xor(lax.axis_index("tp"), k) + 1 for k in range(2)]
        lane = lax.broadcasted_iota(jnp.int32, (16, LANES), 1)
        keep = []
        for tile in range(2):
            past = [lane // 8 + 16 * tile - begin for begin in begins]
            mine = jnp.where(jnp.logical_or((past[0] & -2) == 0, (past[1] & -2) == 0), 1.0, 0.0)
            keep.append(mine.astype(BF16) == 1.0)
        if not given:
            for arrival in arrivals:
                arrival.wait()

        @pl.loop(0, steps)
        def _(i):
            if not given:
                load(i).wait()
            for odd in range(2):
                for p in range(8):
                    turn = 2 * p + odd
                    from_second = turned_slot(turn + begins[1]) <= 1
                    pixel = 8 * odd + p
                    for row in range(0, BLK, 16):
                        some = pl.ds(row, 16)
                        if given:
                            pair = [ref[2 * i + odd, some, :] for ref in (first, second)]
                        else:
                            pair = [both_buf[k, 2 * i + odd, some, :] for k in range(2)]
                        both = jnp.where(from_second, pair[1], pair[0])
                        both = pltpu.roll(both, (LANES - 8 * turn) & 127, 1)
                        out_buf[i, pixel, some, 0:LANES] = jnp.where(keep[0], both, part_buf[i, pixel, some, 0:LANES])
                        high = jnp.where(keep[1][:, 0:64], both[:, 0:64], part_buf[i, pixel, some, LANES:192])
                        out_buf[i, pixel, some, LANES:192] = high
            store(i).start()

        @pl.loop(0, steps)
        def _(i):
            store(i).wait()

        if ahead:
            for i in range(ahead[1]):
                fetch(i).wait()


def patch_call(first, second, result, group0, groups, ahead, part):
    assert group0 % 2 == 0 and groups % 2 == 0
    steps = groups // 2
    given = part is not None
    hbm, vmem = pl.BlockSpec(memory_space=pltpu.HBM), pl.BlockSpec(memory_space=pltpu.VMEM)
    in_specs = ([vmem] * 3 if given else [hbm] * 2) + [hbm]
    operands = [first, second] + ([part] if given else []) + [result]
    out_specs, out_shape = [hbm], [jax.ShapeDtypeStruct((ROWS * COLS, BLK, 192), BF16)]
    scratch = [pltpu.VMEM((steps, 16, BLK, 192), BF16), pltpu.SemaphoreType.DMA((steps,))]
    if not given:
        scratch += [pltpu.VMEM((2, groups, BLK, LANES), BF16), pltpu.SemaphoreType.DMA((2,)), pltpu.SemaphoreType.DMA((steps,))]
    if ahead:
        ahead = (ahead[0], ahead[1] // 2)
        out_specs.append(vmem)
        out_shape.append(pltpu.VMEM((ahead[1], 16, BLK, 192), BF16))
        scratch.append(pltpu.SemaphoreType.DMA((ahead[1],)))
    out = pl.pallas_call(
        functools.partial(patch_body, group0=group0, steps=steps, ahead=ahead, given=given),
        in_specs=in_specs,
        out_specs=out_specs,
        out_shape=out_shape,
        scratch_shapes=scratch,
        input_output_aliases={len(operands) - 1: 0},
        compiler_params=pltpu.CompilerParams(vmem_limit_bytes=PATCH_VMEM_LIMIT),
        cost_estimate=pl.CostEstimate(flops=groups * 10**6, bytes_accessed=groups * 8 * BLK * 192 * 4, transcendentals=0),
    )(*operands)
    return out if ahead else out[0]


def solution(mesh):
    def cross_pairs(k):
        return [(t, 8 + (t ^ k)) for t in range(8)]

    def late_pairs(k):
        return [(8 + t, 8 + (t ^ k)) for t in range(8)]

    def block_step(act_block, w_shard, scale_shard, shift_shard):
        pp, tp = lax.axis_index("pp"), lax.axis_index("tp")

        def send(value, pairs):
            return lax.ppermute(value, ("pp", "tp"), pairs)

        x_rows = jnp.transpose(act_block, (1, 2, 0, 3))
        raw_head = send(head_call(x_rows), cross_pairs(0))
        raw_tail = send(x_rows[HEAD:, :, :RAW], cross_pairs(0))
        w_full = jnp.concatenate([lax.all_gather(w_shard[a], "tp", axis=1, tiled=True) for a in range(3)], axis=0)
        w_full = w_full.reshape(9 * CH, CH)
        affine = lax.all_gather(jnp.stack([scale_shard, shift_shard]), "tp", axis=1, tiled=True)
        scale, shift = affine[0:1], affine[1:2]
        z_meta = jnp.stack([tp, 8 * (3 * tp + 1), 1 - pp]).astype(jnp.int32)
        r_meta = jnp.stack([tp, 24 * tp, pp]).astype(jnp.int32)

        def live(c, after):
            row0, rows = CROSS_CHUNKS[c]
            return conv_call(z_meta, (x_rows,), w_full, scale, shift, after, row0, rows // 2, RAW, LIVE, 2)

        def send_local(c, z_parts):
            base = CROSS_CHUNKS[c][0] // 2 * 7
            return [(g, n, [send(z_parts[k][g - base : g - base + n], cross_pairs(k)) for k in range(2)]) for g, n in LOCAL_CHUNKS[c]]

        def send_cross(z_parts):
            return [send(z_parts[k], cross_pairs(k)) for k in range(2, 8)]

        z_parts = live(0, ())
        local_recv = send_local(0, z_parts)
        z_recv = [send_cross(z_parts)]
        r_parts = conv_call(r_meta, (raw_head, raw_tail), w_full, scale, shift, (), 0, 7, 0, RAW, 4)
        r_recv = [r_parts[0]] + [send(r_parts[k], late_pairs(k)) for k in range(1, 8)]
        z_parts = live(1, (z_parts[0],))
        z_recv.append(send_cross(z_parts))
        local_recv += send_local(1, z_parts)
        result = None
        for (row0, rows), z_parts in zip(CROSS_CHUNKS, z_recv):
            result = merge_call(r_meta, z_parts, r_recv, result, row0, rows)
        parts = {}
        for n, (group0, groups, (first, second)) in enumerate(local_recv):
            ahead = local_recv[n + 2][:2] if n + 2 >= len(local_recv) - FETCHED and n + 2 < len(local_recv) else None
            result = patch_call(first, second, result, group0, groups, ahead, parts.get(n))
            if ahead:
                result, parts[n + 2] = result
        return jnp.transpose(result.reshape(ROWS, COLS, BLK, 192), (3, 0, 1, 2))

    return jax.shard_map(block_step, mesh=mesh, in_specs=(P(("pp", "tp")), P(None, None, "tp", None), P("tp"), P("tp")), out_specs=P("pp", None, None, "tp"), check_vma=False)
```

```python
import functools

import jax
import jax.numpy as jnp
from jax import lax
from jax.experimental import pallas as pl
from jax.experimental.pallas import tpu as pltpu
from jax.sharding import PartitionSpec as P


BF16 = jnp.bfloat16
F32 = jnp.float32
ROWS = 28
COLS = 28
CH = 384
BLK = 48
IMGS = 24
RAW = 8
LIVE = IMGS - RAW
LANES = 128
VMEM_LIMIT = 60 * 1024 * 1024
PATCH_VMEM_LIMIT = 16 * 1024 * 1024
HEAD = 3
FETCHED = 3
CROSS_CHUNKS = ((0, 16), (16, 12))
LOCAL_CHUNKS = (((0, 56),), ((56, 16), (72, 14), (86, 6), (92, 6)))


def head_body(x_ref, out, sem):
    @pl.when(lax.axis_index("pp") == 0)
    def _():
        copy = pltpu.make_async_copy(x_ref.at[pl.ds(0, HEAD), :, pl.ds(0, RAW), :], out, sem)
        copy.start()
        copy.wait()


def head_call(x_rows):
    return pl.pallas_call(
        head_body,
        in_specs=[pl.BlockSpec(memory_space=pltpu.HBM)],
        out_specs=pl.BlockSpec(memory_space=pltpu.VMEM),
        out_shape=pltpu.VMEM((HEAD, COLS, RAW, CH), BF16),
        scratch_shapes=[pltpu.SemaphoreType.DMA],
        compiler_params=pltpu.CompilerParams(vmem_limit_bytes=PATCH_VMEM_LIMIT),
        cost_estimate=pl.CostEstimate(flops=1000, bytes_accessed=HEAD * COLS * RAW * CH * 2, transcendentals=0),
        name="head",
    )(pltpu.with_memory_space_constraint(x_rows, pltpu.HBM))


def conv_body(meta_ref, *refs, **sizes):
    @pl.when(meta_ref[2] == 1)
    def _():
        conv_step(meta_ref, refs, **sizes)


def conv_step(meta_ref, refs, row0, img0, imgs, step_rows, heights):
    outs = refs[-11:-3]
    pad, col, flip = refs[-3:]
    edge = jnp.zeros((imgs, CH), BF16)
    for j in range(step_rows + 2):
        row = step_rows * pl.program_id(0) + row0 - 1 + j

        @pl.when(jnp.logical_or(row < 0, row >= ROWS))
        def _():
            pad[j, 1 : COLS + 1] = jnp.zeros((COLS, imgs, CH), BF16)

        begin = 0
        for piece, height in enumerate(heights):
            row_ref = refs[piece * (step_rows + 2) + j]

            @pl.when(jnp.logical_and(row >= begin, row < begin + height))
            def _():
                pad[j, 1 : COLS + 1] = row_ref[0, :, img0 : img0 + imgs, :]

            begin += height
        pad[j, 0] = edge
        pad[j, COLS + 1] = edge
    w_ref, scale_ref, shift_ref = refs[len(heights) * (step_rows + 2) :][:3]
    size = step_rows * COLS * imgs
    for a in range(3):
        for b in range(3):
            tap = 3 * a + b
            col[:, tap * CH : (tap + 1) * CH] = pad[a : a + step_rows, b : b + COLS].reshape(size, CH)
    pre = jnp.dot(col[...], w_ref[...], preferred_element_type=F32)
    z_val = jnp.maximum(pre * scale_ref[...] + shift_ref[...], 0.0)
    for g in range(size // LANES):
        group = z_val[g * LANES : (g + 1) * LANES]
        if imgs == RAW:
            group = group.reshape(2, 8, 8, CH).swapaxes(0, 1).reshape(LANES, CH)
            turn = meta_ref[1]
        else:
            turn = meta_ref[1] + 8 * ((7 * (row0 // 2 + pl.program_id(0)) + g) % 2)
        flip[g] = pltpu.roll(group, turn, 0).astype(BF16).T
    for k in range(8):
        start = pl.multiple_of(lax.bitwise_xor(meta_ref[0], k) * BLK, BLK)
        for g in range(size // LANES):
            outs[k][g] = flip[g, pl.ds(start, BLK), :]


def conv_call(meta, pieces, w_full, scale, shift, after, row0, steps, img0, imgs, step_rows):
    size = step_rows * COLS * imgs
    groups = size // LANES

    def row_specs(begin, piece):
        height, _, depth, _ = piece.shape
        return [
            pl.BlockSpec((1, COLS, depth, CH), lambda i, m, j=j: (jnp.clip(step_rows * i * m[2] + row0 - 1 + j - begin, 0, height - 1), 0, 0, 0))
            for j in range(step_rows + 2)
        ]

    def whole(*shape):
        return pl.BlockSpec(shape, lambda i, m: (0,) * len(shape))

    heights = tuple(piece.shape[0] for piece in pieces)
    specs, operands, begin = [], [], 0
    for piece in pieces:
        specs += row_specs(begin, piece)
        operands += [piece] * (step_rows + 2)
        begin += piece.shape[0]
    return pl.pallas_call(
        functools.partial(conv_body, row0=row0, img0=img0, imgs=imgs, step_rows=step_rows, heights=heights),
        grid_spec=pltpu.PrefetchScalarGridSpec(
            num_scalar_prefetch=1,
            grid=(steps,),
            in_specs=specs + [whole(9 * CH, CH), whole(1, CH), whole(1, CH)] + [pl.BlockSpec(memory_space=pl.ANY)] * len(after),
            out_specs=[pl.BlockSpec((groups, BLK, LANES), lambda i, m: (i * m[2], 0, 0))] * 8,
            scratch_shapes=[
                pltpu.VMEM((step_rows + 2, COLS + 2, imgs, CH), BF16),
                pltpu.VMEM((size, 9 * CH), BF16),
                pltpu.VMEM((groups, CH, LANES), BF16),
            ],
        ),
        out_shape=[jax.ShapeDtypeStruct((steps * groups, BLK, LANES), BF16)] * 8,
        compiler_params=pltpu.CompilerParams(vmem_limit_bytes=VMEM_LIMIT),
        cost_estimate=pl.CostEstimate(flops=2 * steps * size * 9 * CH * CH, bytes_accessed=steps * size * CH * 4, transcendentals=0),
    )(meta, *operands, w_full, scale, shift, *after)


def turned_slot(turn):
    lane = lax.broadcasted_iota(jnp.int32, (16, LANES), 1)
    return ((lane // 8 - turn) & 15).astype(F32).astype(BF16)


def merge_body(meta_ref, *refs, aliased):
    z_refs, r_refs = refs[0:6], refs[6:14]
    out = refs[15] if aliased else refs[14]
    z_hold, r_hold = refs[-2:]
    slots = ([], [])
    for d in range(8):
        for hold, some in ((r_hold, (3 * d,)), (z_hold, (3 * d + 1, 3 * d + 2))):
            for tile in range(2):
                inside = [s - 16 * tile for s in some if 16 * tile <= s < 16 * tile + 16]
                if inside:
                    slots[tile].append((hold, d, inside[0], len(inside)))

    def merge_pixels(p, odd):
        turn = 2 * p + odd
        slot = turned_slot(turn)
        masks = []
        for tile in range(2):
            for hold, d, begin, count in slots[tile]:
                mask = slot == begin if count == 1 else jnp.logical_and(slot >= begin, slot <= begin + 1)
                masks.append(mask)
        for r in range(7):
            g = 2 * r + odd
            for row in range(0, BLK, 16):
                at = 0
                for tile in range(2):
                    value = None
                    for hold, d, begin, count in slots[tile]:
                        part = hold[d, r if hold is r_hold else g, row : row + 16, :]
                        value = part if value is None else jnp.where(masks[at], part, value)
                        at += 1
                    value = pltpu.roll(value, (LANES - 8 * turn) & 127, 1)
                    if tile == 0:
                        out[8 * g + p, row : row + 16, 0:LANES] = value
                    else:
                        out[8 * g + p, row : row + 16, LANES:192] = value[:, 0:64]

    @pl.when(meta_ref[2] == 1)
    def _():
        for k in range(8):
            d = lax.bitwise_xor(meta_ref[0], k)
            if k >= 2:
                z_hold[d] = z_refs[k - 2][...]
            r_hold[d] = r_refs[k][...]
        for odd in range(2):

            @pl.loop(0, 8)
            def _(p):
                merge_pixels(p, odd)

    @pl.when(meta_ref[2] == 0)
    def _():
        out[...] = jnp.zeros(out.shape, BF16)


def merge_call(meta, z_parts, r_parts, dst, row0, rows):
    quad = row0 // 4
    in_specs = [pl.BlockSpec((14, BLK, LANES), lambda i, m: (i * m[2], 0, 0))] * 6
    in_specs += [pl.BlockSpec((7, BLK, LANES), lambda i, m: (quad + i * m[2], 0, 0))] * 8
    operands = [*z_parts, *r_parts]
    aliases = {}
    if dst is not None:
        in_specs.append(pl.BlockSpec(memory_space=pl.ANY))
        operands.append(dst)
        aliases = {15: 0}
    return pl.pallas_call(
        functools.partial(merge_body, aliased=dst is not None),
        grid_spec=pltpu.PrefetchScalarGridSpec(
            num_scalar_prefetch=1,
            grid=(rows // 4,),
            in_specs=in_specs,
            out_specs=pl.BlockSpec((112, BLK, 192), lambda i, m: (quad + i, 0, 0)),
            scratch_shapes=[pltpu.VMEM((8, 14, BLK, LANES), BF16), pltpu.VMEM((8, 7, BLK, LANES), BF16)],
        ),
        out_shape=jax.ShapeDtypeStruct((ROWS * COLS, BLK, 192), BF16),
        input_output_aliases=aliases,
        compiler_params=pltpu.CompilerParams(vmem_limit_bytes=VMEM_LIMIT),
        cost_estimate=pl.CostEstimate(flops=rows * 10**7, bytes_accessed=rows * COLS * BLK * 192 * 4, transcendentals=0),
    )(meta, *operands)


def patch_body(first, second, *refs, group0, steps, ahead, given):
    refs = list(refs)
    part_buf = refs.pop(0) if given else None
    before, result = refs.pop(0), refs.pop(0)
    fetched, fetch_sem = (refs.pop(0), refs.pop(-1)) if ahead else (None, None)
    out_buf, out_sem = refs[:2]
    if not given:
        both_buf, both_sem, in_sem = refs[2:]
        part_buf = out_buf

    def pixels(start, i):
        return pl.ds(pl.multiple_of(8 * start + 16 * i, 16), 16)

    def load(i):
        return pltpu.make_async_copy(before.at[pixels(group0, i)], part_buf.at[i], in_sem.at[i])

    def store(i):
        return pltpu.make_async_copy(out_buf.at[i], result.at[pixels(group0, i)], out_sem.at[i])

    def fetch(i):
        return pltpu.make_async_copy(before.at[pixels(ahead[0], i)], fetched.at[i], fetch_sem.at[i])

    @pl.when(lax.axis_index("pp") == 1)
    def _():
        if not given:
            arrivals = [pltpu.make_async_copy(ref, both_buf.at[k], both_sem.at[k]) for k, ref in enumerate((first, second))]
            for arrival in arrivals:
                arrival.start()

            @pl.loop(0, steps)
            def _(i):
                load(i).start()

        if ahead:
            for i in range(ahead[1]):
                fetch(i).start()

        begins = [3 * lax.bitwise_xor(lax.axis_index("tp"), k) + 1 for k in range(2)]
        lane = lax.broadcasted_iota(jnp.int32, (16, LANES), 1)
        keep = []
        for tile in range(2):
            past = [lane // 8 + 16 * tile - begin for begin in begins]
            mine = jnp.where(jnp.logical_or((past[0] & -2) == 0, (past[1] & -2) == 0), 1.0, 0.0)
            keep.append(mine.astype(BF16) == 1.0)
        if not given:
            for arrival in arrivals:
                arrival.wait()

        @pl.loop(0, steps)
        def _(i):
            if not given:
                load(i).wait()
            for odd in range(2):
                for p in range(8):
                    turn = 2 * p + odd
                    from_second = turned_slot(turn + begins[1]) <= 1
                    pixel = 8 * odd + p
                    for row in range(0, BLK, 16):
                        some = pl.ds(row, 16)
                        if given:
                            pair = [ref[2 * i + odd, some, :] for ref in (first, second)]
                        else:
                            pair = [both_buf[k, 2 * i + odd, some, :] for k in range(2)]
                        both = jnp.where(from_second, pair[1], pair[0])
                        both = pltpu.roll(both, (LANES - 8 * turn) & 127, 1)
                        out_buf[i, pixel, some, 0:LANES] = jnp.where(keep[0], both, part_buf[i, pixel, some, 0:LANES])
                        high = jnp.where(keep[1][:, 0:64], both[:, 0:64], part_buf[i, pixel, some, LANES:192])
                        out_buf[i, pixel, some, LANES:192] = high
            store(i).start()

        @pl.loop(0, steps)
        def _(i):
            store(i).wait()

        if ahead:
            for i in range(ahead[1]):
                fetch(i).wait()


def patch_call(first, second, result, group0, groups, ahead, part):
    assert group0 % 2 == 0 and groups % 2 == 0
    steps = groups // 2
    given = part is not None
    hbm, vmem = pl.BlockSpec(memory_space=pltpu.HBM), pl.BlockSpec(memory_space=pltpu.VMEM)
    in_specs = ([vmem] * 3 if given else [hbm] * 2) + [hbm]
    operands = [first, second] + ([part] if given else []) + [result]
    out_specs, out_shape = [hbm], [jax.ShapeDtypeStruct((ROWS * COLS, BLK, 192), BF16)]
    scratch = [pltpu.VMEM((steps, 16, BLK, 192), BF16), pltpu.SemaphoreType.DMA((steps,))]
    if not given:
        scratch += [pltpu.VMEM((2, groups, BLK, LANES), BF16), pltpu.SemaphoreType.DMA((2,)), pltpu.SemaphoreType.DMA((steps,))]
    if ahead:
        ahead = (ahead[0], ahead[1] // 2)
        out_specs.append(vmem)
        out_shape.append(pltpu.VMEM((ahead[1], 16, BLK, 192), BF16))
        scratch.append(pltpu.SemaphoreType.DMA((ahead[1],)))
    out = pl.pallas_call(
        functools.partial(patch_body, group0=group0, steps=steps, ahead=ahead, given=given),
        in_specs=in_specs,
        out_specs=out_specs,
        out_shape=out_shape,
        scratch_shapes=scratch,
        input_output_aliases={len(operands) - 1: 0},
        compiler_params=pltpu.CompilerParams(vmem_limit_bytes=PATCH_VMEM_LIMIT),
        cost_estimate=pl.CostEstimate(flops=groups * 10**6, bytes_accessed=groups * 8 * BLK * 192 * 4, transcendentals=0),
    )(*operands)
    return out if ahead else out[0]


def solution(mesh):
    def cross_pairs(k):
        return [(t, 8 + (t ^ k)) for t in range(8)]

    both_pairs = [(t, (t + 8) % 16) for t in range(16)]

    def late_pairs(k):
        return [(8 + t, 8 + (t ^ k)) for t in range(8)]

    def block_step(act_block, w_shard, scale_shard, shift_shard):
        pp, tp = lax.axis_index("pp"), lax.axis_index("tp")

        def send(value, pairs):
            return lax.ppermute(value, ("pp", "tp"), pairs)

        x_rows = jnp.transpose(act_block, (1, 2, 0, 3))
        raw_head = send(head_call(x_rows), both_pairs)
        raw_tail = send(x_rows[HEAD:, :, :RAW], cross_pairs(0))
        w_full = jnp.concatenate([lax.all_gather(w_shard[a], "tp", axis=1, tiled=True) for a in range(3)], axis=0)
        w_full = w_full.reshape(9 * CH, CH)
        affine = lax.all_gather(jnp.stack([scale_shard, shift_shard]), "tp", axis=1, tiled=True)
        scale, shift = affine[0:1], affine[1:2]
        z_meta = jnp.stack([tp, 8 * (3 * tp + 1), 1 - pp]).astype(jnp.int32)
        r_meta = jnp.stack([tp, 24 * tp, pp]).astype(jnp.int32)

        def live(c, after):
            row0, rows = CROSS_CHUNKS[c]
            return conv_call(z_meta, (x_rows,), w_full, scale, shift, after, row0, rows // 2, RAW, LIVE, 2)

        def send_local(c, z_parts):
            base = CROSS_CHUNKS[c][0] // 2 * 7
            return [(g, n, [send(z_parts[k][g - base : g - base + n], cross_pairs(k)) for k in range(2)]) for g, n in LOCAL_CHUNKS[c]]

        def send_cross(z_parts):
            return [send(z_parts[k], cross_pairs(k)) for k in range(2, 8)]

        z_parts = live(0, ())
        local_recv = send_local(0, z_parts)
        z_recv = [send_cross(z_parts)]
        r_parts = conv_call(r_meta, (raw_head, raw_tail), w_full, scale, shift, (), 0, 7, 0, RAW, 4)
        r_recv = [r_parts[0]] + [send(r_parts[k], late_pairs(k)) for k in range(1, 8)]
        z_parts = live(1, (z_parts[0],))
        z_recv.append(send_cross(z_parts))
        local_recv += send_local(1, z_parts)
        result = None
        for (row0, rows), z_parts in zip(CROSS_CHUNKS, z_recv):
            result = merge_call(r_meta, z_parts, r_recv, result, row0, rows)
        parts = {}
        for n, (group0, groups, (first, second)) in enumerate(local_recv):
            ahead = local_recv[n + 2][:2] if n + 2 >= len(local_recv) - FETCHED and n + 2 < len(local_recv) else None
            result = patch_call(first, second, result, group0, groups, ahead, parts.get(n))
            if ahead:
                result, parts[n + 2] = result
        return jnp.transpose(result.reshape(ROWS, COLS, BLK, 192), (3, 0, 1, 2))

    return jax.shard_map(block_step, mesh=mesh, in_specs=(P(("pp", "tp")), P(None, None, "tp", None), P("tp"), P("tp")), out_specs=P("pp", None, None, "tp"), check_vma=False)
```
